32 devices in a mesh: dp: 8 (over z, x), mp: 4 (over y, core).
Axes of the slice: x: 2, y: 2, z: 4, core: 2. Of those that a mesh axis runs over, the one named last changes fastest.
Arguments:
- features: bfloat16 [2048, 512], P('dp'), may hold values from -6 to 6
- adjacency: bfloat16 [64, 32, 128, 128], P('dp'), may hold values from -0.125 to 0.125
- source_block: int32 [64, 32], P('dp'), may hold values from 0 to 1
- edge_type: int32 [64, 32], P('dp'), may hold values from 0 to 19
- target_block: int32 [64, 32], P('dp'), may hold values from 0 to 1
- live_count: int32 [8, 8], P('dp'), may hold values from 24 to 32, as said below
- relation_weight: bfloat16 [20, 512, 512], P(None, None, 'mp'), may hold values from -0.25 to 0.25
- self_weight: bfloat16 [512, 512], P(None, 'mp'), may hold values from -0.25 to 0.25
- layer_bias: bfloat16 [512], P('mp'), may hold values from -3 to 3
- norm_gain: bfloat16 [512], replicated, may hold values from 0.5 to 1.5
Outputs:
- node_states: bfloat16 [2048, 512], P(('dp', 'mp'))
The draws below stay inside these ranges and needn't reach their ends.
Inputs may be any that keep to these rules, and one draw needn't show every extreme that they name: `source_block`: row s * 8 + d names a block among sender s's 2 blocks. `target_block`: row d * 8 + s names a block among receiver d's 2 blocks. live_count[d, s] live slots from sender s to receiver d, the first ones; some receiver has all 32 slots live from every sender.
All inputs are finite; a program needn't handle non-finite values.
Results may differ from the reference program's by a relative error of at most 0.007.
Values may be sent and summed in bfloat16 or wider, within the bound.
No kernel may reach another device: no remote copies, remote signals or barrier semaphores. Data moves between devices by JAX's collectives and lax.ppermute only.
A program may use at most 128 MiB of HBM per device.

```python
import jax
import jax.numpy as jnp
from jax import lax

D = 512
R = 20
BLK = 128
NB_DEV = 2
IN_DEV = 256
PEERS = 8
SLOTS = 32
PAIRS = 64
NODES = 2048


def draw_live_count(key, part):
    lowest = max(1, 3 * SLOTS // 4)
    drawn = jax.random.randint(jax.random.fold_in(key, 11), (PEERS, PEERS), lowest, SLOTS + 1)
    full_row = jax.random.randint(jax.random.fold_in(key, 12), (), 0, PEERS)
    row_index = jnp.arange(PEERS)[:, None]
    return jnp.where(row_index == full_row, SLOTS, drawn).astype(jnp.int32)


def with_ends(values, rng, smallest, largest):
    longest = values.shape.index(max(values.shape))
    spots = []
    for shift in (0, 1):
        where = [jax.random.randint(jax.random.fold_in(rng, axis), (), 0, length) for axis, length in enumerate(values.shape)]
        where[longest] = (where[longest] + shift) % values.shape[longest]
        spots.append(tuple(where))
    return values.at[spots[0]].set(smallest).at[spots[1]].set(largest)


def level_of(key, shape, shards, smallest, largest):
    def one(position, parts):
        draws = jax.random.uniform(jax.random.fold_in(jax.random.fold_in(key, 6), position), (parts,), jnp.float32, smallest / len(shards), largest / len(shards))
        return jnp.repeat(jnp.exp(draws), shape[position] // parts).reshape((-1,) + (1,) * (len(shape) - position - 1))

    factor_of = one(*shards[0])
    for cut in shards[1:]:
        factor_of = factor_of * one(*cut)
    return factor_of


def noise(rng, dims, deviation, limit, cuts=(), held_as=jnp.bfloat16):
    values = jax.random.normal(rng, dims, jnp.float32) * deviation
    if len(cuts) > 0:
        values = level_of(rng, dims, cuts, -0.22, 0.18) * values
    return jnp.clip(values, min=-limit, max=limit).astype(held_as)


def setup_inputs(seed: int = 0) -> dict:
    streams_of = jax.random.split(jax.random.key(seed), 11)
    features = noise(streams_of[0], (NODES, D), 1.0, 6.0, ((0, 8),))
    adjacency = noise(streams_of[1], (PAIRS, SLOTS, BLK, BLK), ((BLK * IN_DEV // NB_DEV) ** -0.5), 0.125, ((0, 8),))
    source_block = with_ends(jax.random.randint(streams_of[2], (PAIRS, SLOTS), 0, NB_DEV), jax.random.fold_in(streams_of[2], 1), 0, NB_DEV - 1).astype(jnp.int32)
    edge_type = with_ends(jax.random.randint(streams_of[3], (PAIRS, SLOTS), 0, R), jax.random.fold_in(streams_of[3], 1), 0, R - 1).astype(jnp.int32)
    target_block = with_ends(jax.random.randint(streams_of[4], (PAIRS, SLOTS), 0, NB_DEV), jax.random.fold_in(streams_of[4], 1), 0, NB_DEV - 1).astype(jnp.int32)
    live_count = draw_live_count(jax.random.fold_in(streams_of[10], 71), 0)
    relation_weight = noise(streams_of[6], (R, D, D), D ** -0.5, 0.25, ((2, 4),))
    self_weight = noise(streams_of[7], (D, D), D ** -0.5, 0.25, ((1, 4),))
    layer_bias = noise(streams_of[8], (D,), 0.5, 3.0, ((0, 4),))
    norm_gain = jnp.clip(1.0 + 0.1 * jax.random.normal(streams_of[9], (D,), jnp.float32), 0.5, 1.5).astype(jnp.bfloat16)
    return dict(features=features, adjacency=adjacency, source_block=source_block, edge_type=edge_type, target_block=target_block, live_count=live_count, relation_weight=relation_weight, self_weight=self_weight, layer_bias=layer_bias, norm_gain=norm_gain)


epsilon = 1e-05

def reference(features, adjacency, source_block, edge_type, target_block, live_count, relation_weight, self_weight, layer_bias, norm_gain):
    stacked = features.reshape(PEERS, NB_DEV, BLK, D)
    adj_tiles = adjacency.reshape(PEERS, PEERS * SLOTS, BLK, BLK)
    lookup_rows = (source_block * R + edge_type).reshape(PEERS, PEERS * SLOTS).astype(jnp.int32)
    active = jnp.arange(SLOTS, dtype=jnp.int32)[None, None, :] < live_count[:, :, None]
    matches = target_block.reshape(PEERS, PEERS, SLOTS)[:, :, :, None] == jnp.arange(NB_DEV, dtype=jnp.int32)[None, None, None, :]
    selector = jnp.logical_and(matches, active[:, :, :, None]).astype(jnp.float32)
    per_sender = jnp.transpose(selector, (1, 0, 2, 3))
    relations = relation_weight.astype(jnp.float32)

    def one_sender(running, inputs):
        block_rows, sender_tiles, sender_rows, sender_select = inputs
        lookup = jnp.einsum('bid,rdc->bric', block_rows.astype(jnp.float32), relations).astype(jnp.bfloat16)
        lookup = lookup.reshape(NB_DEV * R, BLK, D)
        chosen = jnp.take(lookup, sender_rows, axis=0)
        message = jnp.einsum('nij,njc->nic', sender_tiles.astype(jnp.float32), chosen.astype(jnp.float32))
        message = message.reshape(PEERS, SLOTS, BLK * D)
        summed = jnp.einsum('rkb,rkx->rbx', sender_select, message, precision=lax.Precision.HIGHEST)
        return (running + summed, None)
    initial = jnp.zeros((PEERS, NB_DEV, BLK * D), jnp.float32)
    running, ignored = lax.scan(one_sender, initial, (stacked, adj_tiles, lookup_rows, per_sender))
    aggregate = running.reshape(PEERS * NB_DEV * BLK, D)
    own_term = jnp.dot(features, self_weight, preferred_element_type=jnp.float32)
    hidden = jax.nn.relu(own_term + aggregate + layer_bias.astype(jnp.float32)).astype(jnp.bfloat16)
    values = lax.optimization_barrier(hidden).astype(jnp.float32)
    inverse_rms = lax.rsqrt(lax.optimization_barrier(jnp.mean(values * values, axis=1, keepdims=True)) + epsilon)
    return (values * inverse_rms * norm_gain.astype(jnp.float32)).astype(jnp.bfloat16)
```

```python
import jax
import jax.numpy as jnp
from jax import lax
from jax.experimental import pallas as pl
from jax.experimental.pallas import tpu as pltpu
from jax.sharding import PartitionSpec as P

epsilon = 1e-05


def group_of(count, most):
    return max(g for g in range(1, most + 1) if count % g == 0)


def table_kernel(features_ref, weight_ref, self_ref, bias_ref, table_ref, own_ref):
    step = pl.program_id(0)
    group, _, columns = weight_ref.shape
    side = table_ref.shape[1]
    blocks = features_ref.shape[0] // side
    rows = features_ref[...]

    @pl.when(step == 0)
    def _():
        own = jnp.dot(rows, self_ref[...], preferred_element_type=jnp.float32)
        own_ref[...] = own + bias_ref[...].astype(jnp.float32)
        table_ref[table_ref.shape[0] - 1] = jnp.zeros((side, columns), table_ref.dtype)

    wide = jnp.concatenate([weight_ref[g] for g in range(group)], axis=1)
    product = jnp.dot(rows, wide, preferred_element_type=jnp.float32).astype(table_ref.dtype)
    for g in range(group):
        for b in range(blocks):
            table_ref[(step * group + g) * blocks + b] = product[
                b * side : (b + 1) * side, g * columns : (g + 1) * columns
            ]


def message_kernel(me_ref, source_ref, type_ref, target_ref, tiles_ref, table_ref, own_ref, out_ref):
    step = pl.program_id(0)
    receivers, slots, side, _ = tiles_ref.shape
    columns = table_ref.shape[2]
    blocks = out_ref.shape[1] // side
    empty = table_ref.shape[0] - 1
    for d in range(receivers):
        receiver = step * receivers + d
        left = jnp.concatenate([tiles_ref[d, k] for k in range(slots)], axis=1)
        right = []
        for k in range(slots):
            row = type_ref[receiver, k] * blocks + source_ref[receiver, k]
            target = target_ref[receiver, k]
            picked = [table_ref[jnp.where(target == b, row, empty)] for b in range(blocks)]
            right.append(jnp.concatenate(picked, axis=1))
        total = jnp.dot(left, jnp.concatenate(right, axis=0), preferred_element_type=jnp.float32)
        mine = receiver == me_ref[0]
        for b in range(blocks):
            part = slice(b * side, (b + 1) * side)
            piece = total[:, b * columns : (b + 1) * columns]
            out_ref[d, part, :] = (piece + jnp.where(mine, own_ref[part, :], 0.0)).astype(out_ref.dtype)


def finish_kernel(parts_ref, gain_ref, out_ref):
    senders, pieces, rows, columns = parts_ref.shape
    hidden = []
    square = jnp.zeros((rows, 1), jnp.float32)
    for m in range(pieces):
        total = parts_ref[0, m].astype(jnp.float32)
        for s in range(1, senders):
            total = total + parts_ref[s, m].astype(jnp.float32)
        value = jnp.maximum(total, 0.0).astype(jnp.bfloat16).astype(jnp.float32)
        square = square + jnp.sum(value * value, axis=1, keepdims=True)
        hidden.append(value)
    scale = lax.rsqrt(square / (pieces * columns) + epsilon)
    for m in range(pieces):
        part = slice(m * columns, (m + 1) * columns)
        out_ref[:, part] = (hidden[m] * scale * gain_ref[:, part].astype(jnp.float32)).astype(out_ref.dtype)


def per_device(
    features,
    adjacency,
    source_block,
    edge_type,
    target_block,
    live_count,
    relation_weight,
    self_weight,
    layer_bias,
    norm_gain,
):
    peers = lax.axis_size("dp")
    splits = lax.axis_size("mp")
    slots = source_block.shape[1]
    side = adjacency.shape[2]
    node_rows, width = features.shape
    blocks = node_rows // side
    relations, _, columns = relation_weight.shape

    active = jnp.arange(slots, dtype=jnp.int32)[None, :] < live_count.reshape(peers, 1)
    routed = lax.all_to_all(
        jnp.where(active, target_block, blocks), "dp", split_axis=0, concat_axis=0, tiled=True
    )

    group = group_of(relations, 4)
    entries = relations * blocks + 1
    table, own = pl.pallas_call(
        table_kernel,
        grid=(relations // group,),
        in_specs=[
            pl.BlockSpec((node_rows, width), lambda i: (0, 0)),
            pl.BlockSpec((group, width, columns), lambda i: (i, 0, 0)),
            pl.BlockSpec((width, columns), lambda i: (0, 0)),
            pl.BlockSpec((1, columns), lambda i: (0, 0)),
        ],
        out_specs=[
            pl.BlockSpec((entries, side, columns), lambda i: (0, 0, 0)),
            pl.BlockSpec((node_rows, columns), lambda i: (0, 0)),
        ],
        out_shape=[
            jax.ShapeDtypeStruct((entries, side, columns), jnp.bfloat16),
            jax.ShapeDtypeStruct((node_rows, columns), jnp.float32),
        ],
        cost_estimate=pl.CostEstimate(
            flops=2 * node_rows * width * columns * (relations + 1),
            bytes_accessed=2 * (relations * width * columns + entries * side * columns),
            transcendentals=0,
        ),
        name="relation_table",
    )(features, relation_weight, self_weight, layer_bias.reshape(1, columns))

    together = group_of(peers, max(1, 32 // slots))
    smem = pl.BlockSpec(memory_space=pltpu.SMEM)
    partial = pl.pallas_call(
        message_kernel,
        grid=(peers // together,),
        in_specs=[
            smem,
            smem,
            smem,
            smem,
            pl.BlockSpec((together, slots, side, side), lambda i: (i, 0, 0, 0)),
            pl.BlockSpec((entries, side, columns), lambda i: (0, 0, 0)),
            pl.BlockSpec((node_rows, columns), lambda i: (0, 0)),
        ],
        out_specs=pl.BlockSpec((together, node_rows, columns), lambda i: (i, 0, 0)),
        out_shape=jax.ShapeDtypeStruct((peers, node_rows, columns), jnp.bfloat16),
        cost_estimate=pl.CostEstimate(
            flops=2 * peers * slots * side * side * columns * blocks,
            bytes_accessed=2 * (peers * slots * side * side + peers * node_rows * columns),
            transcendentals=0,
        ),
        name="slot_messages",
    )(
        lax.axis_index("dp").astype(jnp.int32).reshape(1),
        source_block,
        edge_type,
        routed,
        adjacency,
        table,
        own,
    )

    arrived = lax.all_to_all(
        partial.reshape(peers * node_rows, columns),
        ("dp", "mp"),
        split_axis=0,
        concat_axis=0,
        tiled=True,
    )
    rows = node_rows // splits
    return pl.pallas_call(
        finish_kernel,
        out_shape=jax.ShapeDtypeStruct((rows, splits * columns), jnp.bfloat16),
        name="sum_and_norm",
    )(arrived.reshape(peers, splits, rows, columns), norm_gain.reshape(1, splits * columns))


def solution(mesh):
    return jax.shard_map(
        per_device,
        mesh=mesh,
        in_specs=(
            P("dp", None),
            P("dp", None, None, None),
            P("dp", None),
            P("dp", None),
            P("dp", None),
            P("dp", None),
            P(None, None, "mp"),
            P(None, "mp"),
            P("mp"),
            P(),
        ),
        out_specs=P(("dp", "mp"), None),
        check_vma=False,
    )
```

```python
import jax
import jax.numpy as jnp
from jax import lax
from jax.experimental import pallas as pl
from jax.experimental.pallas import tpu as pltpu
from jax.sharding import PartitionSpec as P

epsilon = 1e-05
UNROLL = 1
SCRATCH_BYTES = 20 * 1024 * 1024


def on_chip(array):
    return pltpu.with_memory_space_constraint(array, pltpu.VMEM)


def off_chip(array):
    return pltpu.with_memory_space_constraint(array, pltpu.HBM)


def group_of(count, most):
    return max(g for g in range(1, most + 1) if count % g == 0)


def table_kernel(
    features_hbm, weight_hbm, tiles_hbm, table_ref, early_ref,
    features_ref, weight_ref, few_sems, weight_sems,
):
    relations, _, columns = weight_ref.shape
    side = table_ref.shape[1]
    blocks = features_ref.shape[0] // side
    group = group_of(relations, 2)
    chunks = relations // group
    early = early_ref.shape[0]

    halves = 2 if chunks % 2 == 0 else 1
    per_half = chunks // halves

    def weight_copy(half):
        part = pl.ds(half * per_half * group, per_half * group)
        return pltpu.make_async_copy(weight_hbm.at[part], weight_ref.at[part], weight_sems.at[half])

    rows_copy = pltpu.make_async_copy(features_hbm, features_ref, few_sems.at[0])
    early_copy = pltpu.make_async_copy(tiles_hbm.at[pl.ds(0, early)], early_ref, few_sems.at[1])
    rows_copy.start()
    for half in range(halves):
        weight_copy(half).start()
    early_copy.start()
    table_ref[table_ref.shape[0] - 1] = jnp.zeros((side, columns), table_ref.dtype)
    rows_copy.wait()

    def some_relations(step, carry):
        first = step * group
        wide = jnp.concatenate([weight_ref[first + g] for g in range(group)], axis=1)
        product = jnp.dot(features_ref[...], wide, preferred_element_type=jnp.float32)
        product = product.astype(table_ref.dtype)
        for g in range(group):
            for b in range(blocks):
                table_ref[(first + g) * blocks + b] = product[
                    b * side : (b + 1) * side, g * columns : (g + 1) * columns
                ]
        return carry

    for half in range(halves):
        weight_copy(half).wait()
        bounds = (half * per_half, (half + 1) * per_half)
        lax.fori_loop(*bounds, some_relations, 0, unroll=group_of(per_half, 5))
    early_copy.wait()


def message_kernel(
    me_ref, source_ref, type_ref, target_ref, early_ref, tiles_hbm, table_ref,
    features_hbm, self_hbm, bias_hbm, out_ref,
    late_ref, features_ref, self_ref, bias_ref, mine_ref, tile_sems, few_sems,
):
    early, slots, side, _ = early_ref.shape
    receivers = out_ref.shape[0]
    late = receivers - early
    columns = table_ref.shape[2]
    blocks = out_ref.shape[1] // side
    empty = table_ref.shape[0] - 1

    cuts = [0, late - late // 2, late]
    waves = [(cuts[i], cuts[i + 1] - cuts[i]) for i in range(2) if cuts[i + 1] > cuts[i]]

    def wave_copy(wave):
        start, count = waves[wave]
        return pltpu.make_async_copy(
            tiles_hbm.at[pl.ds(early + start, count)], late_ref.at[pl.ds(start, count)], tile_sems.at[wave]
        )

    few = [
        pltpu.make_async_copy(features_hbm, features_ref, few_sems.at[0]),
        pltpu.make_async_copy(self_hbm, self_ref, few_sems.at[1]),
        pltpu.make_async_copy(bias_hbm, bias_ref, few_sems.at[2]),
    ]

    def one_receiver(receiver, tiles_ref, place):
        left = jnp.concatenate([tiles_ref[place, k] for k in range(slots)], axis=1)
        right = []
        for k in range(slots):
            row = type_ref[receiver, k] * blocks + source_ref[receiver, k]
            target = target_ref[receiver, k]
            picked = [table_ref[jnp.where(target == b, row, empty)] for b in range(blocks)]
            right.append(jnp.concatenate(picked, axis=1))
        total = jnp.dot(left, jnp.concatenate(right, axis=0), preferred_element_type=jnp.float32)
        for b in range(blocks):
            part = slice(b * side, (b + 1) * side)
            out_ref[receiver, part, :] = total[:, b * columns : (b + 1) * columns].astype(out_ref.dtype)
        mine_ref[jnp.where(receiver == me_ref[0], 0, 1)] = total

    def first_ones(place, carry):
        one_receiver(place, early_ref, place)
        return carry

    def other_ones(place, carry):
        one_receiver(early + place, late_ref, place)
        return carry

    wave_copy(0).start()
    lax.fori_loop(0, early, first_ones, 0, unroll=group_of(early, UNROLL))
    for wave in range(1, len(waves)):
        wave_copy(wave).start()
    for copy in few:
        copy.start()
    for wave, (start, count) in enumerate(waves):
        wave_copy(wave).wait()
        lax.fori_loop(start, start + count, other_ones, 0, unroll=group_of(count, UNROLL))
    for copy in few:
        copy.wait()
    own = jnp.dot(features_ref[...], self_ref[...], preferred_element_type=jnp.float32)
    own = own + bias_ref[...].astype(jnp.float32)
    for b in range(blocks):
        part = slice(b * side, (b + 1) * side)
        piece = mine_ref[0, :, b * columns : (b + 1) * columns]
        out_ref[me_ref[0], part, :] = (own[part, :] + piece).astype(out_ref.dtype)


def finish_kernel(parts_ref, gain_ref, out_ref):
    senders, pieces, rows, columns = parts_ref.shape
    hidden = []
    square = jnp.zeros((rows, 1), jnp.float32)
    for m in range(pieces):
        total = parts_ref[0, m].astype(jnp.float32)
        for s in range(1, senders):
            total = total + parts_ref[s, m].astype(jnp.float32)
        value = jnp.maximum(total, 0.0).astype(jnp.bfloat16).astype(jnp.float32)
        square = square + jnp.sum(value * value, axis=1, keepdims=True)
        hidden.append(value)
    scale = lax.rsqrt(square / (pieces * columns) + epsilon)
    for m in range(pieces):
        part = slice(m * columns, (m + 1) * columns)
        out_ref[:, part] = (hidden[m] * scale * gain_ref[:, part].astype(jnp.float32)).astype(out_ref.dtype)


def per_device(
    features,
    adjacency,
    source_block,
    edge_type,
    target_block,
    live_count,
    relation_weight,
    self_weight,
    layer_bias,
    norm_gain,
):
    peers = lax.axis_size("dp")
    splits = lax.axis_size("mp")
    slots = source_block.shape[1]
    side = adjacency.shape[2]
    node_rows, width = features.shape
    blocks = node_rows // side
    relations, _, columns = relation_weight.shape

    active = jnp.arange(slots, dtype=jnp.int32)[None, :] < live_count.reshape(peers, 1)
    routed = lax.all_to_all(
        jnp.where(active, target_block, blocks), "dp", split_axis=0, concat_axis=0, tiled=True
    )

    entries = relations * blocks + 1
    early = max(1, peers // 4)
    vmem = pl.BlockSpec(memory_space=pltpu.VMEM)
    smem = pl.BlockSpec(memory_space=pltpu.SMEM)
    hbm = pl.BlockSpec(memory_space=pltpu.HBM)
    params = pltpu.CompilerParams(vmem_limit_bytes=SCRATCH_BYTES)
    table, early_tiles = pl.pallas_call(
        table_kernel,
        in_specs=[hbm] * 3,
        out_specs=[vmem] * 2,
        out_shape=[
            pltpu.VMEM((entries, side, columns), jnp.bfloat16),
            pltpu.VMEM((early, slots, side, side), jnp.bfloat16),
        ],
        scratch_shapes=[
            pltpu.VMEM((node_rows, width), jnp.bfloat16),
            pltpu.VMEM((relations, width, columns), jnp.bfloat16),
            pltpu.SemaphoreType.DMA((2,)),
            pltpu.SemaphoreType.DMA((2,)),
        ],
        cost_estimate=pl.CostEstimate(
            flops=2 * node_rows * width * columns * relations,
            bytes_accessed=2 * (relations * width * columns + early * slots * side * side),
            transcendentals=0,
        ),
        compiler_params=params,
        name="relation_table",
    )(*map(off_chip, (features, relation_weight, adjacency)))

    partial = pl.pallas_call(
        message_kernel,
        in_specs=[smem] * 4 + [vmem, hbm, vmem, hbm, hbm, hbm],
        out_specs=vmem,
        out_shape=jax.ShapeDtypeStruct((peers, node_rows, columns), jnp.bfloat16),
        scratch_shapes=[
            pltpu.VMEM((peers - early, slots, side, side), jnp.bfloat16),
            pltpu.VMEM((node_rows, width), jnp.bfloat16),
            pltpu.VMEM((width, columns), jnp.bfloat16),
            pltpu.VMEM((1, columns), jnp.bfloat16),
            pltpu.VMEM((2, side, blocks * columns), jnp.float32),
            pltpu.SemaphoreType.DMA((2,)),
            pltpu.SemaphoreType.DMA((3,)),
        ],
        cost_estimate=pl.CostEstimate(
            flops=2 * peers * slots * side * side * columns * blocks,
            bytes_accessed=2 * ((peers - early) * slots * side * side + peers * node_rows * columns),
            transcendentals=0,
        ),
        compiler_params=params,
        name="slot_messages",
    )(
        lax.axis_index("dp").astype(jnp.int32).reshape(1),
        source_block,
        edge_type,
        routed,
        on_chip(early_tiles),
        off_chip(adjacency),
        on_chip(table),
        *map(off_chip, (features, self_weight, layer_bias.reshape(1, columns))),
    )

    arrived = lax.all_to_all(
        partial.reshape(peers * node_rows, columns),
        ("dp", "mp"),
        split_axis=0,
        concat_axis=0,
        tiled=True,
    )
    rows = node_rows // splits
    return pl.pallas_call(
        finish_kernel,
        out_shape=jax.ShapeDtypeStruct((rows, splits * columns), jnp.bfloat16),
        compiler_params=params,
        name="sum_and_norm",
    )(on_chip(arrived.reshape(peers, splits, rows, columns)), norm_gain.reshape(1, splits * columns))


def solution(mesh):
    return jax.shard_map(
        per_device,
        mesh=mesh,
        in_specs=(
            P("dp", None),
            P("dp", None, None, None),
            P("dp", None),
            P("dp", None),
            P("dp", None),
            P("dp", None),
            P(None, None, "mp"),
            P(None, "mp"),
            P("mp"),
            P(),
        ),
        out_specs=P(("dp", "mp"), None),
        check_vma=False,
    )
```
